256 devices in a mesh: seq: 64 (over y, z, x_hi), tp: 4 (over x_lo, core).
Axes of the slice: x: 4 (x_hi: 2, x_lo: 2; x = x_hi * 2 + x_lo), y: 4, z: 8, core: 2. Of those that a mesh axis runs over, the one named last changes fastest.
Arguments:
- inputs: bfloat16 [8192, 2048], P(('seq', 'tp')), may hold values from -40 to 40
- gain: float32 [2048], replicated, may hold values from 0.5 to 1.5
- w_gate: bfloat16 [2048, 7168], P('seq', 'tp'), may hold values from -0.125 to 0.125
- w_up: bfloat16 [2048, 7168], P('seq', 'tp'), may hold values from -0.125 to 0.125
- grad_act: bfloat16 [8192, 7168], P('seq', 'tp'), may hold values from -12 to 12
Outputs:
- input_grad: bfloat16 [8192, 2048], P(('seq', 'tp'))
- gain_grad: float32 [2048], replicated
- gate_weight_grad: float32 [2048, 7168], P('seq', 'tp')
The draws below stay inside these ranges and needn't reach their ends.
All inputs are finite; a program needn't handle non-finite values.
Results may differ from the reference program's by a relative error of at most 0.012.
Values may be sent and summed in bfloat16 or wider, within the bound.
No kernel may reach another device: no remote copies, remote signals or barrier semaphores. Data moves between devices by JAX's collectives and lax.ppermute only.
A program may use at most 128 MiB of HBM per device.

```python
import jax
import jax.numpy as jnp
from jax import lax

D = 2048
FF = 7168
TOKENS = 8192


def draw_inputs(key, part):
    first, second = jax.random.split(jax.random.fold_in(key, 11))
    scales = jnp.exp(jax.random.uniform(second, (TOKENS, 1), jnp.float32, 0.0, 2.302585))
    base = jnp.clip(jax.random.normal(first, (TOKENS, D), jnp.float32), -4.0, 4.0)
    return (base * scales).astype(jnp.bfloat16)


def draw_grad_act(key, part):
    first = jax.random.fold_in(jax.random.fold_in(key, 23), 0)
    ramp = 1.0 + 2.0 * jnp.arange(TOKENS, dtype=jnp.float32) / TOKENS
    base = jnp.clip(jax.random.normal(first, (TOKENS, FF), jnp.float32), -4.0, 4.0)
    return (base * ramp[:, None]).astype(jnp.bfloat16)


def block_levels(own_key, dims, cuts, least, high):
    def one(dim, blocks):
        draws = jax.random.uniform(jax.random.fold_in(jax.random.fold_in(own_key, 6), dim), (blocks,), jnp.float32, least / len(cuts), high / len(cuts))
        return jnp.repeat(jnp.exp(draws), dims[dim] // blocks).reshape((-1,) + (1,) * (len(dims) - dim - 1))

    factor_of = one(*cuts[0])
    for cut in cuts[1:]:
        factor_of = factor_of * one(*cut)
    return factor_of


def bell_draw(own_key, shape, spread, bound, cuts=(), kind=jnp.bfloat16):
    loudness = block_levels(own_key, shape, cuts, -0.22, 0.18) if cuts else 1.0
    entries = jax.random.normal(own_key, shape, jnp.float32) * spread * loudness
    return jnp.minimum(jnp.maximum(entries, -bound), bound).astype(kind)


def setup_inputs(seed: int = 0) -> dict:
    streams_of = jax.random.split(jax.random.key(seed), 6)
    return {
        "inputs": draw_inputs(jax.random.fold_in(streams_of[5], 71), 0),
        "gain": jnp.clip(1.0 + 0.1 * jax.random.normal(streams_of[1], (D,), jnp.float32), 0.5, 1.5),
        "w_gate": bell_draw(streams_of[2], (D, FF), D ** -0.5, 0.125, ((0, 64), (1, 4))),
        "w_up": bell_draw(streams_of[3], (D, FF), D ** -0.5, 0.125, ((0, 64), (1, 4))),
        "grad_act": draw_grad_act(jax.random.fold_in(streams_of[5], 71), 0),
    }


def reference(inputs, gain, w_gate, w_up, grad_act):
    values = inputs.astype(jnp.float32)
    inverse = lax.rsqrt(lax.optimization_barrier(jnp.mean(values * values, axis=-1, keepdims=True)) + 1e-05)
    scaled = values * inverse
    normed = (scaled * gain).astype(jnp.bfloat16)
    gate = jnp.dot(normed, w_gate, preferred_element_type=jnp.float32)
    up = jnp.dot(normed, w_up, preferred_element_type=jnp.float32)
    sigmoid_gate = jax.nn.sigmoid(gate)
    cotangent = grad_act.astype(jnp.float32)
    d_up = (cotangent * gate * sigmoid_gate).astype(jnp.bfloat16)
    d_gate = (cotangent * up * sigmoid_gate * (1.0 + gate * (1.0 - sigmoid_gate))).astype(jnp.bfloat16)
    d_normed = jnp.dot(d_gate, w_gate.T, preferred_element_type=jnp.float32) + jnp.dot(d_up, w_up.T, preferred_element_type=jnp.float32)
    gain_grad = lax.optimization_barrier(jnp.sum(d_normed * scaled, axis=0))
    gained = d_normed * gain
    middle = lax.optimization_barrier(jnp.mean(gained * scaled, axis=-1, keepdims=True))
    input_grad = (inverse * (gained - scaled * middle)).astype(jnp.bfloat16)
    gate_weight_grad = jnp.dot(normed.T, d_gate, preferred_element_type=jnp.float32)
    return (input_grad, gain_grad, gate_weight_grad)
```

```python
import jax
import jax.numpy as jnp
from jax import lax
from jax.sharding import Mesh
from jax.sharding import PartitionSpec as P

SHAPE = (4, 2, 2, 2, 2, 2, 2)
AXES = ("y", "z1", "z0", "zv", "xh", "xl", "c")
TP = ("xl", "c")
SEQ = ("y", "z1", "z0", "zv", "xh")
SEQ_TP = SEQ + TP
Z = ("z1", "z0", "zv")
PLANE = ("y", "xl", "xh")
SWAPPED = ("z1", "z0", "zv", "xh", "xl", "c")
HALF = 896


def index_of(bits):
    value = 0
    for bit in bits:
        value = value * 2 + bit
    return value


def all_bits():
    for k in range(64):
        yield tuple((k >> (5 - j)) & 1 for j in range(6))


def piece_pairs(m):
    pairs = []
    for z1, z0, zv, xh, xl, c in all_bits():
        there = (xl, c, xh ^ m, zv, z1, z0)
        pairs.append((index_of((z1, z0, zv, xh, xl, c)), index_of(there)))
    return pairs


def row_pairs():
    pairs = []
    for z1, z0, zv, xh, xl, c in all_bits():
        there = (xh, xl, c, zv, z1, z0)
        pairs.append((index_of((z1, z0, zv, xh, xl, c)), index_of(there)))
    return pairs


def back(pairs):
    return [(b, a) for a, b in pairs]


def move(value, pairs):
    return lax.ppermute(value, SWAPPED, pairs)


def to_peer(value):
    return lax.ppermute(value, "c", [(0, 1), (1, 0)])


def in_order(first, second, flag):
    return jnp.where(flag, second, first), jnp.where(flag, first, second)


def sent_to_all(value, axes):
    peers = lax.axis_size(axes)
    return lax.all_to_all(
        jnp.broadcast_to(value[None], (peers, *value.shape)), axes, 0, 0, tiled=True
    )


def tiles_of(value, parity):
    return jnp.concatenate(
        [value[..., 128 * k : 128 * (k + 1)] for k in range(parity, 16, 2)], axis=-1
    )


def own_first(value, core):
    even, odd = tiles_of(value, 0), tiles_of(value, 1)
    return jnp.concatenate(in_order(even, odd, core), axis=-1)


def as_stored(value, core):
    even, odd = in_order(value[..., :1024], value[..., 1024:], core)
    parts = []
    for k in range(8):
        parts.append(even[..., 128 * k : 128 * (k + 1)])
        parts.append(odd[..., 128 * k : 128 * (k + 1)])
    return jnp.concatenate(parts, axis=-1)


def on_device(inputs, gain, w_gate, w_up, grad_act):
    core = lax.axis_index("c") == 1
    low = lax.axis_index("zv") == 1
    high = lax.axis_index("xh") == 1

    both = jnp.concatenate((w_gate, w_up), axis=0)
    sent = in_order(both[:, :HALF], both[:, HALF:], high)
    got = [move(sent[m], piece_pairs(m)) for m in range(2)]
    own_inputs = move(inputs, row_pairs())
    sent = in_order(grad_act[:, :HALF], grad_act[:, HALF:], high)
    got_act = [move(sent[m], piece_pairs(m)) for m in range(2)]

    first, second = in_order(got[0], got[1], low)
    gate_piece = jnp.concatenate((first[:32], second[:32]), axis=0)
    up_piece = jnp.concatenate((first[32:], second[32:]), axis=0)
    gate_own = sent_to_all(gate_piece, PLANE).reshape(1024, HALF)
    up_own = sent_to_all(up_piece, PLANE).reshape(1024, HALF)
    gate_peer = to_peer(gate_own)
    up_peer = to_peer(up_own)

    own_inputs = own_first(own_inputs, core)
    gain_here = own_first(gain, core)
    values = sent_to_all(own_inputs, Z).reshape(256, 2048).astype(jnp.float32)
    inverse = lax.rsqrt(jnp.mean(values * values, axis=-1, keepdims=True) + 1e-05)
    scaled = values * inverse
    normed = (scaled * gain_here).astype(jnp.bfloat16)
    normed_own, normed_peer = normed[:, :1024], normed[:, 1024:]

    def product(own, peer):
        return jnp.dot(normed_own, own, preferred_element_type=jnp.float32) + jnp.dot(
            normed_peer, peer, preferred_element_type=jnp.float32
        )

    gate = product(gate_own, gate_peer)
    up = product(up_own, up_peer)
    sigmoid_gate = jax.nn.sigmoid(gate)
    cotangent = jnp.concatenate(in_order(got_act[0], got_act[1], low), axis=0).astype(jnp.float32)
    d_up = (cotangent * gate * sigmoid_gate).astype(jnp.bfloat16)
    d_gate = (cotangent * up * sigmoid_gate * (1.0 + gate * (1.0 - sigmoid_gate))).astype(
        jnp.bfloat16
    )

    over_tokens = (((0,), (0,)), ((), ()))
    for_peer = lax.dot_general(
        normed_peer, d_gate, over_tokens, preferred_element_type=jnp.float32
    ).astype(jnp.bfloat16)
    from_peer = to_peer(for_peer)
    for_own = lax.dot_general(normed_own, d_gate, over_tokens, preferred_element_type=jnp.float32)
    chip_grad = (for_own + from_peer.astype(jnp.float32)).astype(jnp.bfloat16)
    arrived = lax.all_to_all(chip_grad.reshape(16, 64, HALF), PLANE, 0, 0, tiled=True)
    rows = arrived.astype(jnp.float32).sum(axis=0).astype(jnp.bfloat16)

    contract = (((1,), (1,)), ((), ()))

    def partial(gate_part, up_part):
        return lax.dot_general(
            d_gate, gate_part, contract, preferred_element_type=jnp.float32
        ) + lax.dot_general(d_up, up_part, contract, preferred_element_type=jnp.float32)

    partial_grad = jnp.concatenate(
        (partial(gate_own, up_own), partial(gate_peer, up_peer)), axis=1
    )
    parts = lax.all_to_all(
        partial_grad.astype(jnp.bfloat16).reshape(8, 32, 2048), Z, 0, 0, tiled=True
    )
    terms = as_stored(jnp.sum(partial_grad * scaled, axis=0), core)
    terms = sent_to_all(terms, ("z1", "z0", "zv", "c")).sum(axis=0)
    gain_grad = sent_to_all(terms, PLANE).sum(axis=0)

    own_grad = parts.astype(jnp.float32).sum(axis=0)
    own_values = own_inputs.astype(jnp.float32)
    own_inverse = lax.rsqrt(jnp.mean(own_values * own_values, axis=-1, keepdims=True) + 1e-05)
    own_scaled = own_values * own_inverse
    gained = own_grad * gain_here
    middle = jnp.mean(gained * own_scaled, axis=-1, keepdims=True)
    own_input_grad = (own_inverse * (gained - own_scaled * middle)).astype(jnp.bfloat16)
    input_grad = move(as_stored(own_input_grad, core), back(row_pairs()))

    sent = in_order(rows[:32], rows[32:], low)
    got = [move(sent[m], back(piece_pairs(m))) for m in range(2)]
    gate_weight_grad = jnp.concatenate(in_order(got[0], got[1], high), axis=1).astype(jnp.float32)
    return (input_grad, gain_grad, gate_weight_grad)


def solution(mesh):
    torus = Mesh(mesh.devices.reshape(SHAPE), AXES)
    placed = (P(SEQ_TP, None), P(), P(SEQ, TP), P(SEQ, TP), P(SEQ, TP))
    return jax.shard_map(
        on_device,
        mesh=torus,
        in_specs=placed,
        out_specs=(P(SEQ_TP, None), P(), P(SEQ, TP)),
        check_vma=False,
    )
```

```python
import jax
import jax.numpy as jnp
from jax import lax
from jax.experimental import pallas as pl
from jax.experimental.pallas import tpu as pltpu
from jax.sharding import Mesh
from jax.sharding import PartitionSpec as P

SHAPE = (4, 2, 2, 2, 2, 2, 2)
AXES = ("y", "z1", "z0", "zv", "xh", "xl", "c")
TP = ("xl", "c")
SEQ = ("y", "z1", "z0", "zv", "xh")
SEQ_TP = SEQ + TP
Z = ("z1", "z0", "zv")
PLANE = ("y", "xh", "xl", "c")
SWAPPED = ("z1", "z0", "zv", "xh", "xl", "c")
HALF = 896
CUTS = ((0, 512), (512, 896))
CLASSES = (2, 4, 3, 12)
BF16, F32 = jnp.bfloat16, jnp.float32


def index_of(bits):
    value = 0
    for bit in bits:
        value = value * 2 + bit
    return value


def all_bits():
    for k in range(64):
        yield tuple((k >> (5 - j)) & 1 for j in range(6))


def pairs_of(there):
    return [(index_of(bits), index_of(there(*bits))) for bits in all_bits()]


def weight_pairs(m1, m0):
    return pairs_of(lambda z1, z0, zv, xh, xl, c: (xl, c, xh ^ m0, z0, z1, zv ^ m1))


def act_pairs(m):
    return pairs_of(lambda z1, z0, zv, xh, xl, c: (xl, c, xh ^ m, z0, z1, zv))


def row_pairs():
    return pairs_of(lambda z1, z0, zv, xh, xl, c: (xh, xl, c, z0, z1, zv))


def back(pairs):
    return [(b, a) for a, b in pairs]


def move(value, pairs):
    return lax.ppermute(value, SWAPPED, pairs)


def to_peer(value):
    return lax.ppermute(value, "c", [(0, 1), (1, 0)])


def class_of(core, color, stage):
    return CLASSES[(stage + 2 * core + color) % 4]


def exchange(value, color, stage):
    pairs = []
    for y in range(4):
        for xh in range(2):
            for xl in range(2):
                for c in range(2):
                    there = (y * 4 + xl * 2 + xh) ^ class_of(c, color, stage)
                    y2, xl2, xh2 = there // 4, (there // 2) % 2, there % 2
                    pairs.append(
                        (((y * 2 + xh) * 2 + xl) * 2 + c, ((y2 * 2 + xh2) * 2 + xl2) * 2 + c)
                    )
    return lax.ppermute(value, PLANE, pairs)


def tiles_in_order():
    core = lax.axis_index("c")
    here = lax.axis_index("y") * 4 + lax.axis_index("xl") * 2 + lax.axis_index("xh")
    flips = []
    for c in range(2):
        for color in range(2):
            for block in range(16):
                flip = 0
                for stage in range(4):
                    if (block >> stage) & 1:
                        flip ^= class_of(c, color, stage)
                flips.append(flip)
    first = jnp.array(flips, jnp.int32)
    second = jnp.array(flips[32:] + flips[:32], jnp.int32)
    return jnp.where(core == 1, second, first) ^ here.astype(jnp.int32)


def in_order(first, second, flag):
    return jnp.where(flag, second, first), jnp.where(flag, first, second)


def sent_to_all(value, axes):
    peers = lax.axis_size(axes)
    return lax.all_to_all(
        jnp.broadcast_to(value[None], (peers, *value.shape)), axes, 0, 0, tiled=True
    )


def tree_sum(value, axes):
    size = lax.axis_size(axes)
    terms = [value]
    for k in range(1, size):
        terms.append(lax.ppermute(value, axes, [(i, i ^ k) for i in range(size)]))
    while len(terms) > 1:
        terms = [terms[k] + terms[k + 1] for k in range(0, len(terms), 2)]
    return terms[0]


def tile_at(tiles_ref, which, color, block):
    return tiles_ref[which * 32 + color * 16 + block]


def act_kernel(tiles_ref, core_ref, normed_ref, act_ref, *refs):
    weights, (mine_ref, peer_ref, gate_ref), (ordered,) = refs[:8], refs[8:11], refs[11:]
    core = core_ref[0] == 1
    for color, (low, high) in enumerate(CUTS):
        width = high - low
        found = []
        for which in range(2):
            for block in range(16):
                at = pl.multiple_of(tile_at(tiles_ref, which, color, block) * 128, 128)
                ordered[:, block * 128 : (block + 1) * 128] = normed_ref[:, pl.ds(at, 128)]
            total = None
            for part in range(2):
                weight = weights[which * 4 + color * 2 + part][...].reshape(1024, width)
                term = jnp.dot(
                    ordered[:, part * 1024 : (part + 1) * 1024],
                    weight,
                    preferred_element_type=F32,
                )
                total = term if total is None else total + term
            found.append(total)
        gate = jnp.where(core, found[1], found[0])
        up = jnp.where(core, found[0], found[1])
        sig = jax.nn.sigmoid(gate)
        cotangent = act_ref[:, low:high].astype(F32)
        d_up = (cotangent * gate * sig).astype(BF16)
        d_gate = (cotangent * up * sig * (1.0 + gate * (1.0 - sig))).astype(BF16)
        gate_ref[:, low:high] = d_gate
        mine_ref[:, low:high] = jnp.where(core, d_up, d_gate)
        peer_ref[:, low:high] = jnp.where(core, d_gate, d_up)


def grad_kernel(tiles_ref, mine_ref, peer_ref, rows_ref, inverse_ref, *refs):
    weights, (out_ref, terms_ref), (total,) = refs[:8], refs[8:10], refs[10:]
    total[...] = jnp.zeros_like(total)
    for which, d_ref in enumerate((mine_ref, peer_ref)):
        for color, (low, high) in enumerate(CUTS):
            for part in range(2):
                weight = weights[which * 4 + color * 2 + part][...].reshape(1024, high - low)
                found = lax.dot_general(
                    d_ref[:, low:high],
                    weight,
                    (((1,), (1,)), ((), ())),
                    preferred_element_type=F32,
                )
                for k in range(8):
                    tile = tile_at(tiles_ref, which, color, part * 8 + k)
                    at = pl.multiple_of(tile * 128, 128)
                    total[:, pl.ds(at, 128)] += found[:, k * 128 : (k + 1) * 128]
    grad = total[...]
    out_ref[...] = grad.astype(BF16)
    scaled = rows_ref[...].astype(F32) * inverse_ref[...]
    terms_ref[...] = jnp.sum(grad * scaled, axis=0, keepdims=True)


def weight_grad_kernel(tiles_ref, core_ref, turned_ref, d_gate_ref, *refs):
    outs, (ordered,) = refs[:4], refs[4:]
    for which in range(2):
        half = (core_ref[0] + which) % 2
        for color, (low, high) in enumerate(CUTS):
            for block in range(16):
                tile = tile_at(tiles_ref, which, color, block)
                at = pl.multiple_of(tile * 128 + half * 64, 64)
                ordered[block * 64 : (block + 1) * 64, :] = turned_ref[pl.ds(at, 64), :]
            found = jnp.dot(ordered[...], d_gate_ref[:, low:high], preferred_element_type=F32)
            outs[which * 2 + color][...] = found.astype(BF16).reshape(16, 64, high - low)


def in_vmem(count):
    return [pl.BlockSpec(memory_space=pltpu.VMEM)] * count


def in_smem(count):
    return [pl.BlockSpec(memory_space=pltpu.SMEM)] * count


def local_call(kernel, shapes, scratch, scalars, arrays, flops):
    return pl.pallas_call(
        kernel,
        out_shape=[jax.ShapeDtypeStruct(*shape) for shape in shapes],
        in_specs=in_smem(len(scalars)) + in_vmem(len(arrays)),
        out_specs=in_vmem(len(shapes)),
        scratch_shapes=scratch,
        cost_estimate=pl.CostEstimate(flops=flops, bytes_accessed=8 << 20, transcendentals=0),
    )(*scalars, *arrays)


def on_device(inputs, gain, w_gate, w_up, grad_act):
    core_index = lax.axis_index("c")
    core = core_index == 1
    low = lax.axis_index("zv") == 1
    high = lax.axis_index("xh") == 1
    tiles = tiles_in_order()
    cores = core_index.astype(jnp.int32).reshape(1)

    gates = in_order(w_gate[:, :HALF], w_gate[:, HALF:], high)
    ups = in_order(w_up[:, :HALF], w_up[:, HALF:], high)
    got = [[None, None], [None, None]]
    for m0 in range(2):
        for m1, piece in enumerate(in_order(gates[m0], ups[m0], low)):
            got[m1][m0] = move(piece, weight_pairs(m1, m0))
    own_inputs = move(inputs, row_pairs())
    sent = in_order(grad_act[:, :HALF], grad_act[:, HALF:], high)
    got_act = [move(sent[m], act_pairs(m)) for m in range(2)]

    by_pair = [jnp.concatenate(in_order(*got[m1], low), axis=0) for m1 in range(2)]
    piece = jnp.concatenate(in_order(*by_pair, core), axis=0)

    weights = [None] * 8
    held = [piece[None, :, a:b] for a, b in CUTS]
    for stage in range(4):
        arrived = [exchange(held[color], color, stage) for color in range(2)]
        if stage < 3:
            held = [jnp.concatenate((held[k], arrived[k]), axis=0) for k in range(2)]
        else:
            for color in range(2):
                for part, value in enumerate((held[color], arrived[color])):
                    weights[color * 2 + part] = value
                    weights[4 + color * 2 + part] = to_peer(value)

    rows = sent_to_all(own_inputs, Z).reshape(256, 2048)
    values = rows.astype(F32)
    inverse = lax.rsqrt(jnp.mean(values * values, axis=-1, keepdims=True) + 1e-05)
    normed = (values * inverse * gain).astype(BF16)
    act = jnp.concatenate(in_order(got_act[0], got_act[1], low), axis=0)

    d_mine, d_peer, d_gate = local_call(
        act_kernel,
        [((256, HALF), BF16)] * 3,
        [pltpu.VMEM((256, 2048), BF16)],
        (tiles, cores),
        (normed, act, *weights),
        4 * 256 * 2048 * HALF,
    )
    partial_grad, terms = local_call(
        grad_kernel,
        [((256, 2048), BF16), ((1, 2048), F32)],
        [pltpu.VMEM((256, 2048), F32)],
        (tiles,),
        (d_mine, d_peer, rows, inverse, *weights),
        4 * 256 * 2048 * HALF,
    )
    parts = lax.all_to_all(partial_grad.reshape(8, 32, 2048), Z, 0, 0, tiled=True)

    grads = local_call(
        weight_grad_kernel,
        [((16, 64, b - a), BF16) for a, b in CUTS + CUTS],
        [pltpu.VMEM((1024, 256), BF16)],
        (tiles, cores),
        (normed.T, d_gate),
        4 * 256 * 2048 * HALF,
    )
    summed = []
    for color in range(2):
        total = grads[color].astype(F32) + to_peer(grads[2 + color]).astype(F32)
        summed.append(total)
    for stage in (3, 2, 1, 0):
        count = 1 << stage
        going = [total.astype(BF16) for total in summed]
        arrived = [exchange(going[k][count:], k, stage) for k in range(2)]
        summed = [summed[k][:count] + arrived[k].astype(F32) for k in range(2)]
    own_rows = jnp.concatenate([total[0].astype(BF16) for total in summed], axis=1)

    gain_grad = terms.reshape(2048)
    for axes in ("c", ("xh", "xl"), "y", Z):
        gain_grad = tree_sum(gain_grad, axes)

    own_grad = parts.astype(F32).sum(axis=0)
    own_values = own_inputs.astype(F32)
    own_inverse = lax.rsqrt(jnp.mean(own_values * own_values, axis=-1, keepdims=True) + 1e-05)
    own_scaled = own_values * own_inverse
    gained = own_grad * gain
    middle = jnp.mean(gained * own_scaled, axis=-1, keepdims=True)
    own_input_grad = (own_inverse * (gained - own_scaled * middle)).astype(BF16)
    input_grad = move(own_input_grad, back(row_pairs()))

    sent = in_order(own_rows[:32], own_rows[32:], low)
    got = [move(sent[m], back(act_pairs(m))) for m in range(2)]
    gate_weight_grad = jnp.concatenate(in_order(got[0], got[1], high), axis=1).astype(F32)
    return (input_grad, gain_grad, gate_weight_grad)


def solution(mesh):
    torus = Mesh(mesh.devices.reshape(SHAPE), AXES)
    placed = (P(SEQ_TP, None), P(), P(SEQ, TP), P(SEQ, TP), P(SEQ, TP))
    return jax.shard_map(
        on_device,
        mesh=torus,
        in_specs=placed,
        out_specs=(P(SEQ_TP, None), P(), P(SEQ, TP)),
        check_vma=False,
    )
```

```python
import jax
import jax.numpy as jnp
from jax import lax
from jax.experimental import pallas as pl
from jax.experimental.pallas import tpu as pltpu
from jax.sharding import Mesh
from jax.sharding import PartitionSpec as P


SHAPE = (4, 2, 2, 2, 2, 2, 2)
AXES = ("y", "z1", "z0", "zv", "xh", "xl", "c")
TP = ("xl", "c")
SEQ = ("y", "z1", "z0", "zv", "xh")
SEQ_TP = SEQ + TP
Z = ("z1", "z0", "zv")
PLANE = ("y", "xh", "xl", "c")
SWAPPED = ("z1", "z0", "zv", "xh", "xl", "c")
HALF = 896
CUTS = ((0, 512), (512, 896))
CLASSES = (2, 4, 3, 12)
BF16, F32 = jnp.bfloat16, jnp.float32


def index_of(bits):
    value = 0
    for bit in bits:
        value = value * 2 + bit
    return value


def all_bits():
    for k in range(64):
        yield tuple((k >> (5 - j)) & 1 for j in range(6))


def pairs_of(there):
    return [(index_of(bits), index_of(there(*bits))) for bits in all_bits()]


def weight_pairs(m1, m0):
    return pairs_of(lambda z1, z0, zv, xh, xl, c: (c, xh ^ m0, xl, z0, z1, zv ^ m1))


def owner_pairs(m):
    return pairs_of(lambda z1, z0, zv, xh, xl, c: (c, xh ^ m, xl, z0, z1, zv))


def act_pairs(m):
    return pairs_of(lambda z1, z0, zv, xh, xl, c: (c, zv ^ m, xl, xh, z1, z0))


def row_pairs():
    return pairs_of(lambda z1, z0, zv, xh, xl, c: (zv, xl, c, xh, z1, z0))


def back(pairs):
    return [(b, a) for a, b in pairs]


def move(value, pairs):
    return lax.ppermute(value, SWAPPED, pairs)


def to_peer(value):
    return lax.ppermute(value, "c", [(0, 1), (1, 0)])


def class_of(core, color, stage):
    return CLASSES[(stage + 2 * core + color) % 4]


def exchange(value, color, stage):
    pairs = []
    for y in range(4):
        for xh in range(2):
            for xl in range(2):
                for c in range(2):
                    there = (y * 4 + xl * 2 + xh) ^ class_of(c, color, stage)
                    y2, xl2, xh2 = there // 4, (there // 2) % 2, there % 2
                    pairs.append(
                        (((y * 2 + xh) * 2 + xl) * 2 + c, ((y2 * 2 + xh2) * 2 + xl2) * 2 + c)
                    )
    return lax.ppermute(value, PLANE, pairs)


def tiles_in_order():
    core = lax.axis_index("c")
    here = lax.axis_index("y") * 4 + lax.axis_index("xl") * 2 + lax.axis_index("xh")
    flips = []
    for c in range(2):
        for color in range(2):
            for block in range(16):
                flip = 0
                for stage in range(4):
                    if (block >> stage) & 1:
                        flip ^= class_of(c, color, stage)
                flips.append(flip)
    first = jnp.array(flips, jnp.int32)
    second = jnp.array(flips[32:] + flips[:32], jnp.int32)
    return jnp.where(core == 1, second, first) ^ here.astype(jnp.int32)


def in_order(first, second, flag):
    return jnp.where(flag, second, first), jnp.where(flag, first, second)


def sent_to_all(value, axes):
    peers = lax.axis_size(axes)
    return lax.all_to_all(
        jnp.broadcast_to(value[None], (peers, *value.shape)), axes, 0, 0, tiled=True
    )


def flip_start(value, axes, flips):
    size = lax.axis_size(axes)
    return [lax.ppermute(value, axes, [(i, i ^ k) for i in range(size)]) for k in flips]


def flip_sum(value, arrived):
    terms = [value, *arrived]
    while len(terms) > 1:
        terms = [terms[k] + terms[k + 1] for k in range(0, len(terms), 2)]
    return terms[0]


def tile_at(tiles_ref, which, color, block):
    return tiles_ref[which * 32 + color * 16 + block]


def rows_kernel(rows_ref, gain_ref, normed_ref, turned_ref, inverse_ref):
    values = rows_ref[...].astype(F32)
    inverse = lax.rsqrt(jnp.mean(values * values, axis=-1, keepdims=True) + 1e-05)
    inverse_ref[...] = inverse
    for k in range(16):
        part = slice(k * 128, (k + 1) * 128)
        scaled = rows_ref[:, part].astype(F32) * inverse
        normed = (scaled * gain_ref[:, part]).astype(BF16)
        normed_ref[:, part] = normed
        turned_ref[part, :] = normed.T


def act_kernel(tiles_ref, core_ref, normed_ref, act_ref, rows_ref, inverse_ref, *refs):
    sources, (gate_ref, out_ref, terms_ref) = refs[:8], refs[8:11]
    weights, (ordered, mine, peer, total, sems) = refs[11:19], refs[19:]
    core = core_ref[0] == 1
    order = [which * 4 + color * 2 + part for color in (0, 1) for which in (0, 1) for part in (0, 1)]
    copies = {k: pltpu.make_async_copy(sources[k], weights[k], sems.at[k]) for k in order}
    for k in order:
        copies[k].start()
    for color, (low, high) in enumerate(CUTS):
        width = high - low
        found = []
        for which in range(2):
            for block in range(16):
                at = pl.multiple_of(tile_at(tiles_ref, which, color, block) * 128, 128)
                ordered[:, block * 128 : (block + 1) * 128] = normed_ref[:, pl.ds(at, 128)]
            sum_of = None
            for part in range(2):
                k = which * 4 + color * 2 + part
                copies[k].wait()
                term = jnp.dot(
                    ordered[:, part * 1024 : (part + 1) * 1024],
                    weights[k][...].reshape(1024, width),
                    preferred_element_type=F32,
                )
                sum_of = term if sum_of is None else sum_of + term
            found.append(sum_of)
        gate = jnp.where(core, found[1], found[0])
        up = jnp.where(core, found[0], found[1])
        sig = jax.nn.sigmoid(gate)
        cotangent = act_ref[:, low:high].astype(F32)
        d_up = (cotangent * gate * sig).astype(BF16)
        d_gate = (cotangent * up * sig * (1.0 + gate * (1.0 - sig))).astype(BF16)
        gate_ref[:, low:high] = d_gate
        mine[:, low:high] = jnp.where(core, d_up, d_gate)
        peer[:, low:high] = jnp.where(core, d_gate, d_up)
    total[...] = jnp.zeros_like(total)
    for which, d_ref in enumerate((mine, peer)):
        for color, (low, high) in enumerate(CUTS):
            for part in range(2):
                weight = weights[which * 4 + color * 2 + part][...].reshape(1024, high - low)
                found = lax.dot_general(
                    d_ref[:, low:high],
                    weight,
                    (((1,), (1,)), ((), ())),
                    preferred_element_type=F32,
                )
                for k in range(8):
                    tile = tile_at(tiles_ref, which, color, part * 8 + k)
                    at = pl.multiple_of(tile * 128, 128)
                    total[:, pl.ds(at, 128)] += found[:, k * 128 : (k + 1) * 128]
    for k in range(16):
        part = slice(k * 128, (k + 1) * 128)
        grad = total[:, part]
        out_ref[:, part] = grad.astype(BF16)
        scaled = rows_ref[:, part].astype(F32) * inverse_ref[...]
        terms_ref[:, part] = jnp.sum(grad * scaled, axis=0, keepdims=True)


def weight_grad_kernel(tiles_ref, core_ref, turned_ref, d_gate_ref, *refs):
    outs, (ordered,) = refs[:4], refs[4:]
    for which in range(2):
        half = (core_ref[0] + which) % 2
        for color, (low, high) in enumerate(CUTS):
            for block in range(16):
                tile = tile_at(tiles_ref, which, color, block)
                at = pl.multiple_of(tile * 128 + half * 64, 64)
                ordered[block * 64 : (block + 1) * 64, :] = turned_ref[pl.ds(at, 64), :]
            found = jnp.dot(ordered[...], d_gate_ref[:, low:high], preferred_element_type=F32)
            outs[which * 2 + color][...] = found.astype(BF16).reshape(16, 64, high - low)


def in_vmem(count):
    return [pl.BlockSpec(memory_space=pltpu.VMEM)] * count


def in_smem(count):
    return [pl.BlockSpec(memory_space=pltpu.SMEM)] * count


def local_call(kernel, shapes, scratch, scalars, arrays, flops, anywhere=()):
    return pl.pallas_call(
        kernel,
        out_shape=[jax.ShapeDtypeStruct(*shape) for shape in shapes],
        in_specs=in_smem(len(scalars))
        + in_vmem(len(arrays))
        + [pl.BlockSpec(memory_space=pl.ANY)] * len(anywhere),
        out_specs=in_vmem(len(shapes)),
        scratch_shapes=scratch,
        cost_estimate=pl.CostEstimate(flops=flops, bytes_accessed=8 << 20, transcendentals=0),
    )(*scalars, *arrays, *anywhere)


def step(inputs, gain, w_gate, w_up, grad_act):
    core_index = lax.axis_index("c")
    core = core_index == 1
    mid = lax.axis_index("z0") == 1
    low = lax.axis_index("zv") == 1
    high = lax.axis_index("xh") == 1
    tiles = tiles_in_order()
    cores = core_index.astype(jnp.int32).reshape(1)

    gates = in_order(w_gate[:, :HALF], w_gate[:, HALF:], high)
    ups = in_order(w_up[:, :HALF], w_up[:, HALF:], high)
    got = [[None, None], [None, None]]
    for m0 in range(2):
        for m1, piece in enumerate(in_order(gates[m0], ups[m0], low)):
            got[m1][m0] = move(piece, weight_pairs(m1, m0))
    own_inputs = move(inputs, row_pairs())
    sent = in_order(grad_act[:, :HALF], grad_act[:, HALF:], low)
    got_act = []
    for m in range(2):
        got_act.append(move(sent[m], act_pairs(m)))

    by_pair = [jnp.concatenate(in_order(*got[m1], mid), axis=0) for m1 in range(2)]
    piece = jnp.concatenate(in_order(*by_pair, core), axis=0)

    weights = [None] * 8
    held = [piece[None, :, a:b] for a, b in CUTS]
    for stage in range(4):
        arrived = []
        for color in range(2):
            arrived.append(exchange(held[color], color, stage))
        arrived = lax.optimization_barrier(arrived)
        if stage < 3:
            held = [jnp.concatenate((held[k], arrived[k]), axis=0) for k in range(2)]
        else:
            for color in range(2):
                for part, value in enumerate((held[color], arrived[color])):
                    weights[color * 2 + part] = value
                    weights[4 + color * 2 + part] = to_peer(value)

    rows = sent_to_all(own_inputs, Z).reshape(256, 2048)
    normed, turned, inverse = local_call(
        rows_kernel,
        [((256, 2048), BF16), ((2048, 256), BF16), ((256, 1), F32)],
        [],
        (),
        (rows, gain.reshape(1, 2048)),
        256 * 2048 * 64,
    )
    act = jnp.concatenate(in_order(got_act[0], got_act[1], mid), axis=0)

    d_gate, partial_grad, terms = local_call(
        act_kernel,
        [((256, HALF), BF16), ((256, 2048), BF16), ((1, 2048), F32)],
        [
            pltpu.VMEM((8, 128, b - a), BF16)
            for a, b in (CUTS[0], CUTS[0], CUTS[1], CUTS[1]) * 2
        ]
        + [
            pltpu.VMEM((256, 2048), BF16),
            pltpu.VMEM((256, HALF), BF16),
            pltpu.VMEM((256, HALF), BF16),
            pltpu.VMEM((256, 2048), F32),
            pltpu.SemaphoreType.DMA((8,)),
        ],
        (tiles, cores),
        (normed, act, rows, inverse),
        8 * 256 * 2048 * HALF,
        weights,
    )
    parts = lax.all_to_all(partial_grad.reshape(8, 32, 2048), Z, 0, 0, tiled=True)

    terms = terms.reshape(2048)
    terms = flip_sum(terms, flip_start(terms, "c", (1,)))
    grads = local_call(
        weight_grad_kernel,
        [((16, 64, b - a), BF16) for a, b in CUTS + CUTS],
        [pltpu.VMEM((1024, 256), BF16)],
        (tiles, cores),
        (turned, d_gate),
        4 * 256 * 2048 * HALF,
    )
    arrived = [to_peer(grads[2 + k]) for k in range(2)]
    flips = flip_start(terms, "xl", (1,))
    *arrived, flipped = lax.optimization_barrier((*arrived, *flips))
    terms = flip_sum(terms, [flipped])
    summed = [grads[k].astype(F32) + arrived[k].astype(F32) for k in range(2)]
    beside = {3: ("y", (1, 2, 3)), 2: ("xh", (1,)), 1: ("zv", (1,)), 0: ("z0", (1,))}
    for stage in (3, 2, 1, 0):
        count = 1 << stage
        going = [total.astype(BF16) for total in summed]
        arrived = [exchange(going[k][count:], k, stage) for k in range(2)]
        flips = flip_start(terms, *beside[stage])
        (*arrived,), (*flips,) = lax.optimization_barrier((tuple(arrived), tuple(flips)))
        terms = flip_sum(terms, flips)
        summed = [summed[k][:count] + arrived[k].astype(F32) for k in range(2)]
    own_rows = jnp.concatenate([total[0].astype(BF16) for total in summed], axis=1)
    sent = in_order(own_rows[:32], own_rows[32:], mid)
    got = [move(sent[m], back(owner_pairs(m))) for m in range(2)]
    gate_weight_grad = jnp.concatenate(in_order(got[0], got[1], high), axis=1).astype(F32)
    gain_grad = flip_sum(terms, flip_start(terms, "z1", (1,)))

    own_grad = parts.astype(F32).sum(axis=0)
    own_values = own_inputs.astype(F32)
    own_inverse = lax.rsqrt(jnp.mean(own_values * own_values, axis=-1, keepdims=True) + 1e-05)
    own_scaled = own_values * own_inverse
    gained = own_grad * gain
    middle = jnp.mean(gained * own_scaled, axis=-1, keepdims=True)
    own_input_grad = (own_inverse * (gained - own_scaled * middle)).astype(BF16)
    input_grad = move(own_input_grad, back(row_pairs()))
    return (input_grad, gain_grad, gate_weight_grad)


def solution(mesh):
    torus = Mesh(mesh.devices.reshape(SHAPE), AXES)
    placed = (P(SEQ_TP, None), P(), P(SEQ, TP), P(SEQ, TP), P(SEQ, TP))
    return jax.shard_map(
        step,
        mesh=torus,
        in_specs=placed,
        out_specs=(P(SEQ_TP, None), P(), P(SEQ, TP)),
        check_vma=False,
    )
```

```python
import jax
import jax.numpy as jnp
from jax import lax
from jax.experimental import pallas as pl
from jax.experimental.pallas import tpu as pltpu
from jax.sharding import Mesh
from jax.sharding import PartitionSpec as P


SHAPE = (4, 2, 2, 2, 2, 2, 2)
AXES = ("y", "z1", "z0", "zv", "xh", "xl", "c")
TP = ("xl", "c")
SEQ = ("y", "z1", "z0", "zv", "xh")
SEQ_TP = SEQ + TP
Z = ("z1", "z0", "zv")
PLANE = ("y", "xh", "xl", "c")
SWAPPED = ("z1", "z0", "zv", "xh", "xl", "c")
HALF = 896
CUTS = ((0, 512), (512, 896))
CLASSES = (2, 4, 3, 12)
BF16, F32 = jnp.bfloat16, jnp.float32


def index_of(bits):
    value = 0
    for bit in bits:
        value = value * 2 + bit
    return value


def all_bits():
    for k in range(64):
        yield tuple((k >> (5 - j)) & 1 for j in range(6))


def pairs_of(there):
    return [(index_of(bits), index_of(there(*bits))) for bits in all_bits()]


def weight_pairs(m1, m0):
    return pairs_of(lambda z1, z0, zv, xh, xl, c: (c, xh ^ m0, xl, z0, z1, zv ^ m1))


def owner_pairs(m):
    return pairs_of(lambda z1, z0, zv, xh, xl, c: (c, xh ^ m, xl, z0, z1, zv))


def act_pairs(m):
    return pairs_of(lambda z1, z0, zv, xh, xl, c: (c, zv ^ m, xl, xh, z1, z0))


def row_pairs():
    return pairs_of(lambda z1, z0, zv, xh, xl, c: (zv, xl, c, xh, z1, z0))


def back(pairs):
    return [(b, a) for a, b in pairs]


def move(value, pairs):
    return lax.ppermute(value, SWAPPED, pairs)


def to_peer(value):
    return lax.ppermute(value, "c", [(0, 1), (1, 0)])


def class_of(core, color, stage):
    return CLASSES[(stage + 2 * core + color) % 4]


def exchange(value, color, stage):
    pairs = []
    for y in range(4):
        for xh in range(2):
            for xl in range(2):
                for c in range(2):
                    there = (y * 4 + xl * 2 + xh) ^ class_of(c, color, stage)
                    y2, xl2, xh2 = there // 4, (there // 2) % 2, there % 2
                    pairs.append(
                        (((y * 2 + xh) * 2 + xl) * 2 + c, ((y2 * 2 + xh2) * 2 + xl2) * 2 + c)
                    )
    return lax.ppermute(value, PLANE, pairs)


def tiles_in_order():
    core = lax.axis_index("c")
    here = lax.axis_index("y") * 4 + lax.axis_index("xl") * 2 + lax.axis_index("xh")
    flips = []
    for c in range(2):
        for color in range(2):
            for block in range(16):
                flip = 0
                for stage in range(4):
                    if (block >> stage) & 1:
                        flip ^= class_of(c, color, stage)
                flips.append(flip)
    first = jnp.array(flips, jnp.int32)
    second = jnp.array(flips[32:] + flips[:32], jnp.int32)
    return jnp.where(core == 1, second, first) ^ here.astype(jnp.int32)


def in_order(first, second, flag):
    return jnp.where(flag, second, first), jnp.where(flag, first, second)


def sent_to_all(value, axes):
    peers = lax.axis_size(axes)
    return lax.all_to_all(
        jnp.broadcast_to(value[None], (peers, *value.shape)), axes, 0, 0, tiled=True
    )


def tile_at(tiles_ref, which, color, block):
    return tiles_ref[which * 32 + color * 16 + block]


def rows_kernel(rows_ref, gain_ref, normed_ref, turned_ref, inverse_ref):
    values = rows_ref[...].astype(F32)
    inverse = lax.rsqrt(jnp.mean(values * values, axis=-1, keepdims=True) + 1e-05)
    inverse_ref[...] = inverse
    for k in range(16):
        part = slice(k * 128, (k + 1) * 128)
        scaled = rows_ref[:, part].astype(F32) * inverse
        normed = (scaled * gain_ref[:, part]).astype(BF16)
        normed_ref[:, part] = normed
        turned_ref[part, :] = normed.T


def act_kernel(
    tiles_ref, core_ref, normed_ref, act_0_ref, act_1_ref, rows_ref, inverse_ref, *refs
):
    sources, (gate_ref, out_ref) = refs[:8], refs[8:10]
    weights, (ordered, mine, peer, total, sems) = refs[10:18], refs[18:]
    core = core_ref[0] == 1
    swapped = core_ref[1] == 1
    order = [which * 4 + color * 2 + part for color in (0, 1) for which in (0, 1) for part in (0, 1)]
    copies = {k: pltpu.make_async_copy(sources[k], weights[k], sems.at[k]) for k in order}
    for k in order:
        copies[k].start()
    for color, (low, high) in enumerate(CUTS):
        width = high - low
        found = []
        for which in range(2):
            for block in range(16):
                at = pl.multiple_of(tile_at(tiles_ref, which, color, block) * 128, 128)
                ordered[:, block * 128 : (block + 1) * 128] = normed_ref[:, pl.ds(at, 128)]
            sum_of = None
            for part in range(2):
                k = which * 4 + color * 2 + part
                copies[k].wait()
                term = jnp.dot(
                    ordered[:, part * 1024 : (part + 1) * 1024],
                    weights[k][...].reshape(1024, width),
                    preferred_element_type=F32,
                )
                sum_of = term if sum_of is None else sum_of + term
            found.append(sum_of)
        gate = jnp.where(core, found[1], found[0])
        up = jnp.where(core, found[0], found[1])
        sig = jax.nn.sigmoid(gate)
        first = act_0_ref[:, low:high].astype(F32)
        second = act_1_ref[:, low:high].astype(F32)
        cotangent = jnp.concatenate(in_order(first, second, swapped), axis=0)
        d_up = (cotangent * gate * sig).astype(BF16)
        d_gate = (cotangent * up * sig * (1.0 + gate * (1.0 - sig))).astype(BF16)
        gate_ref[:, low:high] = d_gate
        mine[:, low:high] = jnp.where(core, d_up, d_gate)
        peer[:, low:high] = jnp.where(core, d_gate, d_up)
    total[...] = jnp.zeros_like(total)
    for which, d_ref in enumerate((mine, peer)):
        for color, (low, high) in enumerate(CUTS):
            for part in range(2):
                weight = weights[which * 4 + color * 2 + part][...].reshape(1024, high - low)
                found = lax.dot_general(
                    d_ref[:, low:high],
                    weight,
                    (((1,), (1,)), ((), ())),
                    preferred_element_type=F32,
                )
                for k in range(8):
                    tile = tile_at(tiles_ref, which, color, part * 8 + k)
                    at = pl.multiple_of(tile * 128, 128)
                    total[:, pl.ds(at, 128)] += found[:, k * 128 : (k + 1) * 128]
    terms = []
    for k in range(16):
        part = slice(k * 128, (k + 1) * 128)
        grad = total[:, part]
        out_ref[:, part] = grad.astype(BF16)
        scaled = rows_ref[:, part].astype(F32) * inverse_ref[...]
        terms.append(jnp.sum(grad * scaled, axis=0, keepdims=True))
    for k in range(8):
        found = []
        left = terms[2 * k : 2 * k + 2]
        for _ in range(3):
            sent = [value.astype(BF16).astype(F32) for value in left]
            left = [value - gone for value, gone in zip(left, sent)]
            found.extend(sent)
        found.append(jnp.zeros((26, 128), F32))
        out_ref[32 * k : 32 * (k + 1), 2048:] = jnp.concatenate(found, axis=0).astype(BF16)


def weight_grad_kernel(tiles_ref, core_ref, turned_ref, d_gate_ref, *refs):
    outs, (ordered,) = refs[:4], refs[4:]
    for which in range(2):
        half = (core_ref[0] + which) % 2
        for color, (low, high) in enumerate(CUTS):
            for block in range(16):
                tile = tile_at(tiles_ref, which, color, block)
                at = pl.multiple_of(tile * 128 + half * 64, 64)
                ordered[block * 64 : (block + 1) * 64, :] = turned_ref[pl.ds(at, 64), :]
            found = jnp.dot(ordered[...], d_gate_ref[:, low:high], preferred_element_type=F32)
            outs[which * 2 + color][...] = found.astype(BF16).reshape(16, 64, high - low)


def in_vmem(count):
    return [pl.BlockSpec(memory_space=pltpu.VMEM)] * count


def in_smem(count):
    return [pl.BlockSpec(memory_space=pltpu.SMEM)] * count


def local_call(kernel, shapes, scratch, scalars, arrays, flops, anywhere=()):
    return pl.pallas_call(
        kernel,
        out_shape=[jax.ShapeDtypeStruct(*shape) for shape in shapes],
        in_specs=in_smem(len(scalars))
        + in_vmem(len(arrays))
        + [pl.BlockSpec(memory_space=pl.ANY)] * len(anywhere),
        out_specs=in_vmem(len(shapes)),
        scratch_shapes=scratch,
        cost_estimate=pl.CostEstimate(flops=flops, bytes_accessed=8 << 20, transcendentals=0),
    )(*scalars, *arrays, *anywhere)


def step(inputs, gain, w_gate, w_up, grad_act):
    core_index = lax.axis_index("c")
    core = core_index == 1
    mid = lax.axis_index("z0") == 1
    low = lax.axis_index("zv") == 1
    high = lax.axis_index("xh") == 1
    tiles = tiles_in_order()
    cores = jnp.stack((core_index, lax.axis_index("z0"))).astype(jnp.int32)

    gates = in_order(w_gate[:, :HALF], w_gate[:, HALF:], high)
    ups = in_order(w_up[:, :HALF], w_up[:, HALF:], high)
    got = [[None, None], [None, None]]
    for m0 in range(2):
        for m1, piece in enumerate(in_order(gates[m0], ups[m0], low)):
            got[m1][m0] = move(piece, weight_pairs(m1, m0))
    own_inputs = move(inputs, row_pairs())
    sent = in_order(grad_act[:, :HALF], grad_act[:, HALF:], low)
    got_act = []
    for m in range(2):
        got_act.append(move(sent[m], act_pairs(m)))

    by_pair = [jnp.concatenate(in_order(*got[m1], mid), axis=0) for m1 in range(2)]
    piece = jnp.concatenate(in_order(*by_pair, core), axis=0)

    weights = [None] * 8
    held = [piece[None, :, a:b] for a, b in CUTS]
    for stage in range(4):
        arrived = []
        for color in range(2):
            arrived.append(exchange(held[color], color, stage))
        arrived = lax.optimization_barrier(arrived)
        if stage < 3:
            held = [jnp.concatenate((held[k], arrived[k]), axis=0) for k in range(2)]
        else:
            for color in range(2):
                for part, value in enumerate((held[color], arrived[color])):
                    weights[color * 2 + part] = value
                    weights[4 + color * 2 + part] = to_peer(value)

    rows = sent_to_all(own_inputs, Z).reshape(256, 2048)
    normed, turned, inverse = local_call(
        rows_kernel,
        [((256, 2048), BF16), ((2048, 256), BF16), ((256, 1), F32)],
        [],
        (),
        (rows, gain.reshape(1, 2048)),
        256 * 2048 * 64,
    )
    d_gate, partial_grad = local_call(
        act_kernel,
        [((256, HALF), BF16), ((256, 2176), BF16)],
        [
            pltpu.VMEM((8, 128, b - a), BF16)
            for a, b in (CUTS[0], CUTS[0], CUTS[1], CUTS[1]) * 2
        ]
        + [
            pltpu.VMEM((256, 2048), BF16),
            pltpu.VMEM((256, HALF), BF16),
            pltpu.VMEM((256, HALF), BF16),
            pltpu.VMEM((256, 2048), F32),
            pltpu.SemaphoreType.DMA((8,)),
        ],
        (tiles, cores),
        (normed, got_act[0], got_act[1], rows, inverse),
        8 * 256 * 2048 * HALF,
        weights,
    )
    parts = lax.all_to_all(partial_grad.reshape(8, 32, 2176), Z, 0, 0, tiled=True)

    grads = local_call(
        weight_grad_kernel,
        [((16, 64, b - a), BF16) for a, b in CUTS + CUTS],
        [pltpu.VMEM((1024, 256), BF16)],
        (tiles, cores),
        (turned, d_gate),
        4 * 256 * 2048 * HALF,
    )
    arrived = [to_peer(grads[2 + k]) for k in range(2)]
    arrived = lax.optimization_barrier(arrived)
    summed = [grads[k].astype(F32) + arrived[k].astype(F32) for k in range(2)]
    for stage in (3, 2, 1, 0):
        count = 1 << stage
        going = [total.astype(BF16) for total in summed]
        arrived = [exchange(going[k][count:], k, stage) for k in range(2)]
        arrived = lax.optimization_barrier(arrived)
        summed = [summed[k][:count] + arrived[k].astype(F32) for k in range(2)]
    own_rows = jnp.concatenate([total[0].astype(BF16) for total in summed], axis=1)
    sent = in_order(own_rows[:32], own_rows[32:], mid)
    got = [move(sent[m], back(owner_pairs(m))) for m in range(2)]
    gate_weight_grad = jnp.concatenate(in_order(got[0], got[1], high), axis=1).astype(F32)

    terms = parts[:, :6, 2048:].astype(F32).sum(axis=0).reshape(3, 256).sum(axis=0)
    terms = sent_to_all(terms, PLANE).sum(axis=0)
    gain_grad = sent_to_all(terms, Z).reshape(2048)

    own_grad = parts[:, :, :2048].astype(F32).sum(axis=0)
    own_values = own_inputs.astype(F32)
    own_inverse = lax.rsqrt(jnp.mean(own_values * own_values, axis=-1, keepdims=True) + 1e-05)
    own_scaled = own_values * own_inverse
    gained = own_grad * gain
    middle = jnp.mean(gained * own_scaled, axis=-1, keepdims=True)
    own_input_grad = (own_inverse * (gained - own_scaled * middle)).astype(BF16)
    input_grad = move(own_input_grad, back(row_pairs()))
    return (input_grad, gain_grad, gate_weight_grad)


def solution(mesh):
    torus = Mesh(mesh.devices.reshape(SHAPE), AXES)
    placed = (P(SEQ_TP, None), P(), P(SEQ, TP), P(SEQ, TP), P(SEQ, TP))
    return jax.shard_map(
        step,
        mesh=torus,
        in_specs=placed,
        out_specs=(P(SEQ_TP, None), P(), P(SEQ, TP)),
        check_vma=False,
    )
```

```python
import jax
import jax.numpy as jnp
from jax import lax
from jax.experimental import pallas as pl
from jax.experimental.pallas import tpu as pltpu
from jax.sharding import Mesh
from jax.sharding import PartitionSpec as P


SHAPE = (4, 2, 2, 2, 2, 2, 2)
AXES = ("y", "z1", "z0", "zv", "xh", "xl", "c")
TP = ("xl", "c")
SEQ = ("y", "z1", "z0", "zv", "xh")
SEQ_TP = SEQ + TP
Z = ("z1", "z0", "zv")
PLANE = ("y", "xh", "xl", "c")
SWAPPED = ("z1", "z0", "zv", "xh", "xl", "c")
HALF = 896
CUTS = ((0, 512), (512, 896))
CLASSES = (2, 4, 3, 12)
BF16, F32 = jnp.bfloat16, jnp.float32


def index_of(bits):
    value = 0
    for bit in bits:
        value = value * 2 + bit
    return value


def all_bits():
    for k in range(64):
        yield tuple((k >> (5 - j)) & 1 for j in range(6))


def pairs_of(there):
    return [(index_of(bits), index_of(there(*bits))) for bits in all_bits()]


def weight_pairs(m1, m0):
    return pairs_of(lambda z1, z0, zv, xh, xl, c: (c, xh ^ m0, xl, z0, z1, zv ^ m1))


def owner_pairs(m):
    return pairs_of(lambda z1, z0, zv, xh, xl, c: (c, xh ^ m, xl, z0, z1, zv))


def act_pairs(m):
    return pairs_of(lambda z1, z0, zv, xh, xl, c: (c, zv ^ m, xl, xh, z1, z0))


def row_pairs():
    return pairs_of(lambda z1, z0, zv, xh, xl, c: (zv, xl, c, xh, z1, z0))


def back(pairs):
    return [(b, a) for a, b in pairs]


def move(value, pairs):
    return lax.ppermute(value, SWAPPED, pairs)


def to_peer(value):
    return lax.ppermute(value, "c", [(0, 1), (1, 0)])


def class_of(core, color, stage):
    return CLASSES[(stage + 2 * core + color) % 4]


def exchange(value, color, stage):
    pairs = []
    for y in range(4):
        for xh in range(2):
            for xl in range(2):
                for c in range(2):
                    there = (y * 4 + xl * 2 + xh) ^ class_of(c, color, stage)
                    y2, xl2, xh2 = there // 4, (there // 2) % 2, there % 2
                    pairs.append(
                        (((y * 2 + xh) * 2 + xl) * 2 + c, ((y2 * 2 + xh2) * 2 + xl2) * 2 + c)
                    )
    return lax.ppermute(value, PLANE, pairs)


def tiles_in_order():
    core = lax.axis_index("c")
    here = lax.axis_index("y") * 4 + lax.axis_index("xl") * 2 + lax.axis_index("xh")
    flips = []
    for c in range(2):
        for color in range(2):
            for block in range(16):
                flip = 0
                for stage in range(4):
                    if (block >> stage) & 1:
                        flip ^= class_of(c, color, stage)
                flips.append(flip)
    first = jnp.array(flips, jnp.int32)
    second = jnp.array(flips[32:] + flips[:32], jnp.int32)
    return jnp.where(core == 1, second, first) ^ here.astype(jnp.int32)


def in_order(first, second, flag):
    return jnp.where(flag, second, first), jnp.where(flag, first, second)


def sent_to_all(value, axes):
    peers = lax.axis_size(axes)
    return lax.all_to_all(
        jnp.broadcast_to(value[None], (peers, *value.shape)), axes, 0, 0, tiled=True
    )


FLIPS = (("z1", 1), ("z0", 1), ("y", 1), ("y", 3), ("xh", 1), ("xl", 1), ("zv", 1), ("c", 1))


def flipped(value, k):
    axis, flip = FLIPS[k]
    pairs = [(i, i ^ flip) for i in range(lax.axis_size(axis))]
    return value + lax.ppermute(value, axis, pairs)


def tile_at(tiles_ref, which, color, block):
    return tiles_ref[which * 32 + color * 16 + block]


def rows_kernel(rows_ref, gain_ref, normed_ref, turned_ref, inverse_ref):
    values = rows_ref[...].astype(F32)
    inverse = lax.rsqrt(jnp.mean(values * values, axis=-1, keepdims=True) + 1e-05)
    inverse_ref[...] = inverse
    for k in range(16):
        part = slice(k * 128, (k + 1) * 128)
        scaled = rows_ref[:, part].astype(F32) * inverse
        normed = (scaled * gain_ref[:, part]).astype(BF16)
        normed_ref[:, part] = normed
        turned_ref[part, :] = normed.T


def act_kernel(
    tiles_ref, core_ref, normed_ref, act_0_ref, act_1_ref, rows_ref, inverse_ref, *refs
):
    sources, (gate_ref, out_ref, terms_ref) = refs[:8], refs[8:11]
    weights, (ordered, mine, peer, total, sems) = refs[11:19], refs[19:]
    core = core_ref[0] == 1
    swapped = core_ref[1] == 1
    order = [which * 4 + color * 2 + part for color in (0, 1) for which in (0, 1) for part in (0, 1)]
    copies = {k: pltpu.make_async_copy(sources[k], weights[k], sems.at[k]) for k in order}
    for k in order:
        copies[k].start()
    for color, (low, high) in enumerate(CUTS):
        width = high - low
        found = []
        for which in range(2):
            for block in range(16):
                at = pl.multiple_of(tile_at(tiles_ref, which, color, block) * 128, 128)
                ordered[:, block * 128 : (block + 1) * 128] = normed_ref[:, pl.ds(at, 128)]
            sum_of = None
            for part in range(2):
                k = which * 4 + color * 2 + part
                copies[k].wait()
                term = jnp.dot(
                    ordered[:, part * 1024 : (part + 1) * 1024],
                    weights[k][...].reshape(1024, width),
                    preferred_element_type=F32,
                )
                sum_of = term if sum_of is None else sum_of + term
            found.append(sum_of)
        gate = jnp.where(core, found[1], found[0])
        up = jnp.where(core, found[0], found[1])
        sig = jax.nn.sigmoid(gate)
        first = act_0_ref[:, low:high].astype(F32)
        second = act_1_ref[:, low:high].astype(F32)
        cotangent = jnp.concatenate(in_order(first, second, swapped), axis=0)
        d_up = (cotangent * gate * sig).astype(BF16)
        d_gate = (cotangent * up * sig * (1.0 + gate * (1.0 - sig))).astype(BF16)
        gate_ref[:, low:high] = d_gate
        mine[:, low:high] = jnp.where(core, d_up, d_gate)
        peer[:, low:high] = jnp.where(core, d_gate, d_up)
    total[...] = jnp.zeros_like(total)
    for which, d_ref in enumerate((mine, peer)):
        for color, (low, high) in enumerate(CUTS):
            for part in range(2):
                weight = weights[which * 4 + color * 2 + part][...].reshape(1024, high - low)
                found = lax.dot_general(
                    d_ref[:, low:high],
                    weight,
                    (((1,), (1,)), ((), ())),
                    preferred_element_type=F32,
                )
                for k in range(8):
                    tile = tile_at(tiles_ref, which, color, part * 8 + k)
                    at = pl.multiple_of(tile * 128, 128)
                    total[:, pl.ds(at, 128)] += found[:, k * 128 : (k + 1) * 128]
    for k in range(16):
        part = slice(k * 128, (k + 1) * 128)
        grad = total[:, part]
        out_ref[:, part] = grad.astype(BF16)
        scaled = rows_ref[:, part].astype(F32) * inverse_ref[...]
        terms_ref[:, part] = jnp.sum(grad * scaled, axis=0, keepdims=True)


def weight_grad_kernel(tiles_ref, core_ref, turned_ref, d_gate_ref, *refs):
    outs, (ordered,) = refs[:4], refs[4:]
    for which in range(2):
        half = (core_ref[0] + which) % 2
        for color, (low, high) in enumerate(CUTS):
            for block in range(16):
                tile = tile_at(tiles_ref, which, color, block)
                at = pl.multiple_of(tile * 128 + half * 64, 64)
                ordered[block * 64 : (block + 1) * 64, :] = turned_ref[pl.ds(at, 64), :]
            found = jnp.dot(ordered[...], d_gate_ref[:, low:high], preferred_element_type=F32)
            outs[which * 2 + color][...] = found.astype(BF16).reshape(16, 64, high - low)


def in_vmem(count):
    return [pl.BlockSpec(memory_space=pltpu.VMEM)] * count


def in_smem(count):
    return [pl.BlockSpec(memory_space=pltpu.SMEM)] * count


def local_call(kernel, shapes, scratch, scalars, arrays, flops, anywhere=()):
    return pl.pallas_call(
        kernel,
        out_shape=[jax.ShapeDtypeStruct(*shape) for shape in shapes],
        in_specs=in_smem(len(scalars))
        + in_vmem(len(arrays))
        + [pl.BlockSpec(memory_space=pl.ANY)] * len(anywhere),
        out_specs=in_vmem(len(shapes)),
        scratch_shapes=scratch,
        cost_estimate=pl.CostEstimate(flops=flops, bytes_accessed=8 << 20, transcendentals=0),
    )(*scalars, *arrays, *anywhere)


def step(inputs, gain, w_gate, w_up, grad_act):
    core_index = lax.axis_index("c")
    core = core_index == 1
    mid = lax.axis_index("z0") == 1
    low = lax.axis_index("zv") == 1
    high = lax.axis_index("xh") == 1
    tiles = tiles_in_order()
    cores = jnp.stack((core_index, lax.axis_index("z0"))).astype(jnp.int32)

    gates = in_order(w_gate[:, :HALF], w_gate[:, HALF:], high)
    ups = in_order(w_up[:, :HALF], w_up[:, HALF:], high)
    got = [[None, None], [None, None]]
    for m0 in range(2):
        for m1, piece in enumerate(in_order(gates[m0], ups[m0], low)):
            got[m1][m0] = move(piece, weight_pairs(m1, m0))
    own_inputs = move(inputs, row_pairs())
    sent = in_order(grad_act[:, :HALF], grad_act[:, HALF:], low)
    got_act = []
    for m in range(2):
        got_act.append(move(sent[m], act_pairs(m)))

    by_pair = [jnp.concatenate(in_order(*got[m1], mid), axis=0) for m1 in range(2)]
    piece = jnp.concatenate(in_order(*by_pair, core), axis=0)

    weights = [None] * 8
    held = [piece[None, :, a:b] for a, b in CUTS]
    for stage in range(4):
        arrived = []
        for color in range(2):
            arrived.append(exchange(held[color], color, stage))
        arrived = lax.optimization_barrier(arrived)
        if stage < 3:
            held = [jnp.concatenate((held[k], arrived[k]), axis=0) for k in range(2)]
        else:
            for color in range(2):
                for part, value in enumerate((held[color], arrived[color])):
                    weights[color * 2 + part] = value
                    weights[4 + color * 2 + part] = to_peer(value)

    rows = sent_to_all(own_inputs, Z).reshape(256, 2048)
    normed, turned, inverse = local_call(
        rows_kernel,
        [((256, 2048), BF16), ((2048, 256), BF16), ((256, 1), F32)],
        [],
        (),
        (rows, gain.reshape(1, 2048)),
        256 * 2048 * 64,
    )
    d_gate, partial_grad, terms = local_call(
        act_kernel,
        [((256, HALF), BF16), ((256, 2048), BF16), ((1, 2048), F32)],
        [
            pltpu.VMEM((8, 128, b - a), BF16)
            for a, b in (CUTS[0], CUTS[0], CUTS[1], CUTS[1]) * 2
        ]
        + [
            pltpu.VMEM((256, 2048), BF16),
            pltpu.VMEM((256, HALF), BF16),
            pltpu.VMEM((256, HALF), BF16),
            pltpu.VMEM((256, 2048), F32),
            pltpu.SemaphoreType.DMA((8,)),
        ],
        (tiles, cores),
        (normed, got_act[0], got_act[1], rows, inverse),
        8 * 256 * 2048 * HALF,
        weights,
    )
    parts = lax.all_to_all(partial_grad.reshape(8, 32, 2048), Z, 0, 0, tiled=True)

    terms = flipped(terms.reshape(2048), 0)
    grads = local_call(
        weight_grad_kernel,
        [((16, 64, b - a), BF16) for a, b in CUTS + CUTS],
        [pltpu.VMEM((1024, 256), BF16)],
        (tiles, cores),
        (turned, d_gate),
        4 * 256 * 2048 * HALF,
    )
    arrived = []
    for color in range(2):
        arrived.append(to_peer(grads[2 + color]))
    *arrived, terms = lax.optimization_barrier((*arrived, flipped(terms, 1)))
    summed = [grads[k].astype(F32) + arrived[k].astype(F32) for k in range(2)]
    for stage in (3, 2, 1, 0):
        count = 1 << stage
        going = [total.astype(BF16) for total in summed]
        arrived = []
        for color in range(2):
            arrived.append(exchange(going[color][count:], color, stage))
        *arrived, terms = lax.optimization_barrier((*arrived, flipped(terms, 5 - stage)))
        summed = [summed[k][:count] + arrived[k].astype(F32) for k in range(2)]
    own_rows = jnp.concatenate([total[0].astype(BF16) for total in summed], axis=1)
    sent = in_order(own_rows[:32], own_rows[32:], mid)
    got = []
    for m in range(2):
        got.append(move(sent[m], back(owner_pairs(m))))
    gate_weight_grad = jnp.concatenate(in_order(got[0], got[1], high), axis=1).astype(F32)

    gain_grad = flipped(flipped(terms, 6), 7)

    own_grad = parts.astype(F32).sum(axis=0)
    own_values = own_inputs.astype(F32)
    own_inverse = lax.rsqrt(jnp.mean(own_values * own_values, axis=-1, keepdims=True) + 1e-05)
    own_scaled = own_values * own_inverse
    gained = own_grad * gain
    middle = jnp.mean(gained * own_scaled, axis=-1, keepdims=True)
    own_input_grad = (own_inverse * (gained - own_scaled * middle)).astype(BF16)
    input_grad = move(own_input_grad, back(row_pairs()))
    return (input_grad, gain_grad, gate_weight_grad)


def solution(mesh):
    torus = Mesh(mesh.devices.reshape(SHAPE), AXES)
    placed = (P(SEQ_TP, None), P(), P(SEQ, TP), P(SEQ, TP), P(SEQ, TP))
    return jax.shard_map(
        step,
        mesh=torus,
        in_specs=placed,
        out_specs=(P(SEQ_TP, None), P(), P(SEQ, TP)),
        check_vma=False,
    )
```
